32 devices in a mesh: pr: 4 (over y, x), pc: 8 (over z, core).
Axes of the slice: x: 2, y: 2, z: 4, core: 2. Of those that a mesh axis runs over, the one named last changes fastest.
Arguments:
- pair_state: bfloat16 [96, 96, 128], P('pr', 'pc'), may hold values from -6 to 6
- left_weight: bfloat16 [128, 128], replicated, may hold values from -0.5 to 0.5
- right_weight: bfloat16 [128, 128], replicated, may hold values from -0.5 to 0.5
- mid_gain: float32 [128], replicated, may hold values from 0.25 to 1.75
- out_weight: bfloat16 [128, 128], replicated, may hold values from -0.5 to 0.5
- out_gate: bfloat16 [128, 128], replicated, may hold values from -0.5 to 0.5
Outputs:
- pair_update: bfloat16 [96, 96, 128], P('pr', 'pc')
The draws below stay inside these ranges and needn't reach their ends.
All inputs are finite; a program needn't handle non-finite values.
Results may differ from the reference program's by a relative error of at most 0.012.
Values may be sent and summed in bfloat16 or wider, within the bound.
No kernel may reach another device: no remote copies, remote signals or barrier semaphores. Data moves between devices by JAX's collectives and lax.ppermute only.
A program may use at most 128 MiB of HBM per device.

```python
import jax
import jax.numpy as jnp
from jax import lax

RESIDUES = 96
PAIR_WIDTH = 128
MIX_WIDTH = 128


def levels(stream_key, dims, pieces, smallest, top_value):
    level, own = 1.0, jax.random.fold_in(stream_key, 6)
    for dim, shards_of in pieces:
        heights = jnp.exp(jax.random.uniform(jax.random.fold_in(own, dim), (shards_of,), jnp.float32, smallest / len(pieces), top_value / len(pieces)))
        level = level * jnp.repeat(heights, dims[dim] // shards_of).reshape([-1 if axis == dim else 1 for axis in range(len(dims))])
    return level


def scatter_about(key, shape, spread, limit, shards=(), kind=jnp.bfloat16):
    array = spread * jax.random.normal(key, shape, jnp.float32)
    if shards:
        array = array * levels(key, shape, shards, -0.22, 0.18)
    return jnp.clip(array, -limit, limit).astype(kind)


def setup_inputs(seed: int = 0) -> dict:
    keys = jax.random.split(jax.random.key(seed), 7)
    pair_state = scatter_about(keys[0], (RESIDUES, RESIDUES, PAIR_WIDTH), 1.0, 6.0, ((0, 4), (1, 8)))
    left_weight = scatter_about(keys[1], (PAIR_WIDTH, MIX_WIDTH), PAIR_WIDTH ** -0.5, 0.5)
    right_weight = scatter_about(keys[2], (PAIR_WIDTH, MIX_WIDTH), PAIR_WIDTH ** -0.5, 0.5)
    mid_gain = jnp.clip(1.0 + 0.15 * jax.random.normal(keys[3], (MIX_WIDTH,), jnp.float32), 0.25, 1.75)
    out_weight = scatter_about(keys[4], (MIX_WIDTH, PAIR_WIDTH), MIX_WIDTH ** -0.5, 0.5)
    out_gate = scatter_about(keys[5], (PAIR_WIDTH, PAIR_WIDTH), PAIR_WIDTH ** -0.5, 0.5)
    return dict(pair_state=pair_state, left_weight=left_weight, right_weight=right_weight, mid_gain=mid_gain, out_weight=out_weight, out_gate=out_gate)


def scale_channels(values, channel_gain):
    centred = values - lax.optimization_barrier(jnp.mean(values, axis=-1, keepdims=True))
    return centred * lax.rsqrt(lax.optimization_barrier(jnp.mean(centred * centred, axis=-1, keepdims=True)) + 1e-05) * channel_gain

def project_pair(pair_in, left_weight, right_weight):
    ready = pair_in
    left = jnp.einsum('ijc,cd->ijd', ready.astype(jnp.float32), left_weight.astype(jnp.float32))
    right = jnp.einsum('ijc,cd->ijd', ready.astype(jnp.float32), right_weight.astype(jnp.float32))
    return (ready, left.astype(jnp.bfloat16), right.astype(jnp.bfloat16))

def close_update(mixed, ready, mid_gain, out_weight, out_gate):
    scaled = scale_channels(mixed.astype(jnp.float32), mid_gain).astype(jnp.bfloat16)
    scaled = lax.optimization_barrier(scaled)
    gate = jax.nn.sigmoid(jnp.einsum('ijc,cd->ijd', ready.astype(jnp.float32), out_gate.astype(jnp.float32)))
    return (jnp.einsum('ijd,dc->ijc', scaled.astype(jnp.float32), out_weight.astype(jnp.float32)) * gate).astype(jnp.bfloat16)

def reference(pair_state, left_weight, right_weight, mid_gain, out_weight, out_gate):
    ready, left, right = project_pair(pair_state, left_weight, right_weight)
    left, right = lax.optimization_barrier((left, right))

    def one_channel(pair_of):
        return (jnp.dot(pair_of[0].T, pair_of[1], preferred_element_type=jnp.float32) * RESIDUES ** (-0.5)).astype(jnp.bfloat16)
    mixed = jnp.moveaxis(lax.map(one_channel, (jnp.moveaxis(left, -1, 0), jnp.moveaxis(right, -1, 0))), 0, -1)
    mixed = lax.optimization_barrier(mixed)
    return close_update(mixed, ready, mid_gain, out_weight, out_gate)
```

```python
import math

import jax
import jax.numpy as jnp
from jax import lax
from jax.experimental import pallas as pl
from jax.experimental.pallas import tpu as pltpu
from jax.sharding import PartitionSpec as P

VMEM = pl.BlockSpec(memory_space=pltpu.VMEM)


def partner(place, step, count):
    if count & (count - 1) == 0:
        return place ^ abs(step)
    return (place - step) % count


def sum_kernel(spread, ways, seconds, firsts):
    rows = seconds * firsts
    lines = ways * seconds
    tall = math.gcd(lines, 24)
    wide = math.gcd(seconds, 12)
    deep = math.gcd(firsts, 8)

    def kernel(*refs):
        lefts, own, left_weight, right_weight = refs[:ways], *refs[ways : ways + 3]
        outs = refs[ways + 3 : ways + 3 + spread]
        left_rows, right_rows = refs[ways + 3 + spread :]
        row = lax.axis_index("pr")
        place = lax.axis_index("pc")
        line, lane = place // ways, place % ways

        def product(block, weight):
            return (
                jnp.dot(block, weight[...], preferred_element_type=jnp.float32)
                .astype(jnp.bfloat16)
                .astype(jnp.float32)
            )

        right_rows[...] = product(own[...], right_weight)
        for step in range(spread):
            target = partner(row, -step, spread)
            slot = line ^ target if spread & (spread - 1) == 0 else (line - target) % spread
            for turn in range(ways):
                start = pl.multiple_of(partner(lane, turn, ways) * rows, 8)
                left_rows[pl.ds(start, rows), :] = product(lefts[turn][slot], left_weight)
            for top in range(0, lines, tall):
                for first in range(0, seconds, wide):

                    def some(turn, sums):
                        for inner in range(deep):
                            k = turn * deep + inner
                            left = left_rows[pl.ds(top * firsts + k, tall, stride=firsts), :]
                            sums = tuple(
                                total + left * right_rows[pl.ds((first + j) * firsts + k, 1), :]
                                for j, total in enumerate(sums)
                            )
                        return sums

                    zero = jnp.zeros((tall, 128), jnp.float32)
                    sums = lax.fori_loop(0, firsts // deep, some, (zero,) * wide)
                    for j, total in enumerate(sums):
                        at = (first + j) * lines + top
                        outs[step][pl.ds(at, tall), :] = total.astype(outs[step].dtype)

    return kernel


def close_kernel(parts, scale):
    def kernel(*refs):
        sums, (own, gain, out_weight, out_gate, out) = refs[:parts], refs[parts:]
        total = sums[0][...]
        for part in sums[1:]:
            total = total + part[...].astype(jnp.float32)
        mixed = (total * scale).astype(jnp.bfloat16).astype(jnp.float32)
        centred = mixed - jnp.mean(mixed, axis=-1, keepdims=True)
        power = jnp.mean(centred * centred, axis=-1, keepdims=True)
        scaled = (centred * lax.rsqrt(power + 1e-05) * gain[...]).astype(jnp.bfloat16)
        gate = jax.nn.sigmoid(jnp.dot(own[...], out_gate[...], preferred_element_type=jnp.float32))
        update = jnp.dot(scaled, out_weight[...], preferred_element_type=jnp.float32)
        out[...] = (update * gate).astype(out.dtype)

    return kernel


def body(pair_state, left_weight, right_weight, mid_gain, out_weight, out_gate):
    firsts, seconds, width = pair_state.shape
    spread, across = lax.axis_size("pr"), lax.axis_size("pc")
    ways = across // spread
    mixes = left_weight.shape[1]
    rows = seconds * firsts
    own = jnp.transpose(pair_state, (1, 0, 2)).reshape(rows, width)

    def along(step):
        return [
            (partner(line, step, spread) * ways + lane, line * ways + lane)
            for line in range(spread)
            for lane in range(ways)
        ]

    def beside(step):
        return [
            (line * ways + partner(lane, step, ways), line * ways + lane)
            for line in range(spread)
            for lane in range(ways)
        ]

    lines = jnp.stack([own] + [lax.ppermute(own, "pc", along(s)) for s in range(1, spread)])
    lefts = [lines] + [lax.ppermute(lines, "pc", beside(t)) for t in range(1, ways)]
    out_shape = [
        jax.ShapeDtypeStruct((rows, mixes), jnp.float32 if s == 0 else jnp.bfloat16)
        for s in range(spread)
    ]
    sums = pl.pallas_call(
        sum_kernel(spread, ways, seconds, firsts),
        out_shape=out_shape,
        in_specs=[VMEM] * (ways + 3),
        out_specs=[VMEM] * spread,
        scratch_shapes=[
            pltpu.VMEM((ways * rows, mixes), jnp.float32),
            pltpu.VMEM((rows, mixes), jnp.float32),
        ],
        name="sums",
    )(*lefts, own, left_weight, right_weight)
    parts = [sums[0]] + [
        lax.ppermute(
            sums[s], "pr", [(partner(row, s, spread), row) for row in range(spread)]
        )
        for s in range(1, spread)
    ]
    update = pl.pallas_call(
        close_kernel(spread, (spread * firsts) ** -0.5),
        out_shape=jax.ShapeDtypeStruct((rows, width), pair_state.dtype),
        in_specs=[VMEM] * (spread + 4),
        out_specs=VMEM,
        name="close",
    )(*parts, own, mid_gain.reshape(1, mixes), out_weight, out_gate)
    return jnp.transpose(update.reshape(seconds, firsts, width), (1, 0, 2))


def solution(mesh):
    placed = (P("pr", "pc", None), P(), P(), P(), P(), P())
    return jax.shard_map(
        body, mesh=mesh, in_specs=placed, out_specs=P("pr", "pc", None), check_vma=False
    )
```

```python
import math

import jax
import jax.numpy as jnp
from jax import lax
from jax.experimental import pallas as pl
from jax.experimental.pallas import tpu as pltpu
from jax.sharding import PartitionSpec as P

VMEM = pl.BlockSpec(memory_space=pltpu.VMEM)
F32, BF16 = jnp.float32, jnp.bfloat16


def partner(place, step, count):
    if count & (count - 1) == 0:
        return place ^ abs(step)
    return (place - step) % count


def step_from(place, source, count):
    return place ^ source if count & (count - 1) == 0 else (place - source) % count


def product(block, weight):
    return jnp.dot(block, weight, preferred_element_type=F32).astype(BF16).astype(F32)


class Sums:
    def __init__(self, ways, seconds, firsts):
        self.ways, self.seconds, self.firsts = ways, seconds, firsts
        self.rows = seconds * firsts
        self.tile = seconds * seconds
        self.scratch = [
            pltpu.VMEM((self.rows, 128), F32),
            pltpu.VMEM((ways * self.tile, 128), F32),
        ]

    def run(self, block, weight, rights, lefts, sums):
        seconds, firsts = self.seconds, self.firsts
        lines = self.ways * seconds
        tall, wide, deep = math.gcd(lines, 24), math.gcd(seconds, 12), math.gcd(firsts, 8)
        lefts[...] = product(block, weight)
        for top in range(0, lines, tall):
            for first in range(0, seconds, wide):

                def some(turn, totals):
                    for inner in range(deep):
                        k = turn * deep + inner
                        right = rights[pl.ds(top * firsts + k, tall, stride=firsts), :]
                        totals = tuple(
                            total + right * lefts[pl.ds((first + i) * firsts + k, 1), :]
                            for i, total in enumerate(totals)
                        )
                    return totals

                zero = jnp.zeros((tall, 128), F32)
                totals = lax.fori_loop(0, firsts // deep, some, (zero,) * wide)
                for i, total in enumerate(totals):
                    for lane in range(top // seconds, -(-(top + tall) // seconds)):
                        low = max(top, lane * seconds)
                        high = min(top + tall, (lane + 1) * seconds)
                        at = lane * self.tile + (first + i) * seconds + low - lane * seconds
                        sums[at : at + high - low, :] = total[low - top : high - top]


def open_kernel(plan):
    def kernel(*refs):
        ways, rows = plan.ways, plan.rows
        owns, (left_w, right_w, gain, out_w, out_gate) = refs[:ways], refs[ways : ways + 5]
        rights, part, gate, gain_out, weight_out, lefts, sums = refs[ways + 5 :]
        lane = lax.axis_index("pc") % ways
        for turn in range(ways):
            start = pl.multiple_of(partner(lane, turn, ways) * rows, 8)
            rights[pl.ds(start, rows), :] = product(owns[turn][...], right_w[...])
        plan.run(owns[0][...], left_w[...], rights, lefts, sums)
        part[...] = sums[...].astype(BF16)
        gate[...] = jax.nn.sigmoid(
            jnp.dot(owns[0][...], out_gate[...], preferred_element_type=F32)
        )
        gain_out[...] = gain[...]
        weight_out[...] = out_w[...]

    return kernel


def step_kernel(plan):
    def kernel(block, left_w, rights, part, lefts, sums):
        plan.run(block[...], left_w[...], rights, lefts, sums)
        part[...] = sums[...].astype(BF16)

    return kernel


def last_kernel(plan, spread, order):
    def kernel(*refs):
        ways, tile = plan.ways, plan.tile
        block, left_w, rights = refs[:3]
        parts, outs = refs[3 : 2 + spread], refs[2 + spread : 2 + spread + spread * ways]
        lefts, sums, held = refs[2 + spread + spread * ways :]
        for step, part in zip(order[:-1], parts):
            held[step] = part[...].astype(F32)
        plan.run(block[...], left_w[...], rights, lefts, held.at[order[-1]])
        row = lax.axis_index("pr")
        place = lax.axis_index("pc")
        line, lane = place // ways, place % ways
        for step in range(spread):
            slot = step_from(line, partner(row, -step, spread), spread)
            for turn in range(ways):
                start = pl.multiple_of(partner(lane, -turn, ways) * tile, 8)
                out = outs[step * ways + turn]
                out[...] = held[slot, pl.ds(start, tile), :].astype(BF16)

    return kernel


def close_kernel(plan, spread, scale):
    def kernel(*refs):
        ways, seconds, firsts, tile = plan.ways, plan.seconds, plan.firsts, plan.tile
        parts, (gate, gain, out_w, out, mixes, ordered) = refs[: spread * ways], refs[spread * ways :]
        lane = lax.axis_index("pc") % ways
        for turn in range(ways):
            total = parts[turn][...].astype(F32)
            for step in range(1, spread):
                total = total + parts[step * ways + turn][...].astype(F32)
            start = pl.multiple_of(partner(lane, turn, ways) * tile, 8)
            mixes[pl.ds(start, tile), :] = total * scale
        for j in range(seconds):
            ordered[j * firsts : (j + 1) * firsts, :] = mixes[pl.ds(j, firsts, stride=seconds), :]
        mixed = ordered[...].astype(BF16).astype(F32)
        centred = mixed - jnp.mean(mixed, axis=-1, keepdims=True)
        power = jnp.mean(centred * centred, axis=-1, keepdims=True)
        scaled = (centred * lax.rsqrt(power + 1e-05) * gain[...]).astype(BF16)
        update = jnp.dot(scaled, out_w[...], preferred_element_type=F32)
        out[...] = (update * gate[...]).astype(out.dtype)

    return kernel


def body(pair_state, left_weight, right_weight, mid_gain, out_weight, out_gate):
    firsts, seconds, width = pair_state.shape
    spread, across = lax.axis_size("pr"), lax.axis_size("pc")
    ways = across // spread
    mixes = left_weight.shape[1]
    rows = seconds * firsts
    plan = Sums(ways, seconds, firsts)
    own = jnp.transpose(pair_state, (1, 0, 2)).reshape(rows, width)

    def send(values, row_step, line_step, lane_step):
        def at(row, line, lane):
            return row * across + line * ways + lane

        pairs = [
            (
                at(
                    partner(row, row_step, spread),
                    partner(line, line_step, spread),
                    partner(lane, lane_step, ways),
                ),
                at(row, line, lane),
            )
            for row in range(spread)
            for line in range(spread)
            for lane in range(ways)
        ]
        return lax.ppermute(values, ("pr", "pc"), pairs)

    def call(kernel, shapes, scratch, name, *operands):
        return pl.pallas_call(
            kernel,
            out_shape=[jax.ShapeDtypeStruct(shape, kind) for shape, kind in shapes],
            in_specs=[VMEM] * len(operands),
            out_specs=[VMEM] * len(shapes),
            scratch_shapes=scratch,
            name=name,
        )(*operands)

    moved = {step: send(own, 0, step, 0) for step in range(1, spread)}
    owns = [own] + [send(own, 0, 0, turn) for turn in range(1, ways)]
    order = [0, spread - 1] + [step for step in range(1, spread - 1)]
    part_shape = (ways * plan.tile, mixes)
    rights, part, gate, gain, weight = call(
        open_kernel(plan),
        [
            ((ways * rows, mixes), F32),
            (part_shape, BF16),
            ((rows, width), F32),
            ((1, mixes), F32),
            (out_weight.shape, BF16),
        ],
        plan.scratch,
        "open",
        *owns,
        left_weight,
        right_weight,
        mid_gain.reshape(1, mixes),
        out_weight,
        out_gate,
    )
    parts = [part]
    for step in order[1:-1]:
        parts += call(
            step_kernel(plan),
            [(part_shape, BF16)],
            plan.scratch,
            "step",
            moved[step],
            left_weight,
            rights,
        )
    outs = call(
        last_kernel(plan, spread, order),
        [((plan.tile, mixes), BF16)] * (spread * ways),
        plan.scratch + [pltpu.VMEM((spread,) + part_shape, F32)],
        "last",
        moved[order[-1]],
        left_weight,
        rights,
        *parts,
    )
    met = [
        outs[step * ways + turn] if step == turn == 0 else send(outs[step * ways + turn], step, 0, turn)
        for step in range(spread)
        for turn in range(ways)
    ]
    (update,) = call(
        close_kernel(plan, spread, (spread * firsts) ** -0.5),
        [((rows, width), BF16)],
        [pltpu.VMEM((ways * plan.tile, mixes), F32), pltpu.VMEM((rows, mixes), F32)],
        "close",
        *met,
        gate,
        gain,
        weight,
    )
    return jnp.transpose(update.reshape(seconds, firsts, width), (1, 0, 2))


def solution(mesh):
    placed = (P("pr", "pc", None), P(), P(), P(), P(), P())
    return jax.shard_map(
        body, mesh=mesh, in_specs=placed, out_specs=P("pr", "pc", None), check_vma=False
    )
```

```python
import math

import jax
import jax.numpy as jnp
from jax import lax
from jax.experimental import pallas as pl
from jax.experimental.pallas import tpu as pltpu
from jax.sharding import PartitionSpec as P

VMEM = pl.BlockSpec(memory_space=pltpu.VMEM)
F32, BF16 = jnp.float32, jnp.bfloat16


def partner(place, step, count):
    if count & (count - 1) == 0:
        return place ^ abs(step)
    return (place - step) % count


def step_from(place, source, count):
    return place ^ source if count & (count - 1) == 0 else (place - source) % count


def product(block, weight):
    return jnp.dot(block, weight, preferred_element_type=F32).astype(BF16).astype(F32)


class Sums:
    def __init__(self, ways, seconds, firsts):
        self.ways, self.seconds, self.firsts = ways, seconds, firsts
        self.rows = seconds * firsts
        self.tile = seconds * seconds
        self.scratch = [
            pltpu.VMEM((self.rows, 128), F32),
            pltpu.VMEM((ways * self.tile, 128), F32),
        ]

    def run(self, block, weight, rights, lefts, sums):
        seconds, firsts = self.seconds, self.firsts
        lines = self.ways * seconds
        tall, wide, deep = math.gcd(lines, 24), math.gcd(seconds, 12), math.gcd(firsts, 8)
        lefts[...] = product(block, weight)
        for top in range(0, lines, tall):
            for first in range(0, seconds, wide):

                def some(turn, totals):
                    for inner in range(deep):
                        k = turn * deep + inner
                        right = rights[pl.ds(top * firsts + k, tall, stride=firsts), :]
                        totals = tuple(
                            total + right * lefts[pl.ds((first + i) * firsts + k, 1), :]
                            for i, total in enumerate(totals)
                        )
                    return totals

                zero = jnp.zeros((tall, 128), F32)
                totals = lax.fori_loop(0, firsts // deep, some, (zero,) * wide)
                for i, total in enumerate(totals):
                    for lane in range(top // seconds, -(-(top + tall) // seconds)):
                        low = max(top, lane * seconds)
                        high = min(top + tall, (lane + 1) * seconds)
                        at = lane * self.tile + (first + i) * seconds + low - lane * seconds
                        sums[at : at + high - low, :] = total[low - top : high - top]


def open_kernel(plan):
    def kernel(*refs):
        ways, rows = plan.ways, plan.rows
        owns, (left_w, right_w, gain, out_w, out_gate) = refs[:ways], refs[ways : ways + 5]
        rights, part, gate, gain_out, weight_out, lefts, sums = refs[ways + 5 :]
        lane = lax.axis_index("pc") % ways
        for turn in range(ways):
            start = pl.multiple_of(partner(lane, turn, ways) * rows, 8)
            rights[pl.ds(start, rows), :] = product(owns[turn][...], right_w[...])
        plan.run(owns[0][...], left_w[...], rights, lefts, sums)
        part[...] = sums[...].astype(BF16)
        gate[...] = jax.nn.sigmoid(
            jnp.dot(owns[0][...], out_gate[...], preferred_element_type=F32)
        )
        gain_out[...] = gain[...]
        weight_out[...] = out_w[...]

    return kernel


def step_kernel(plan):
    def kernel(block, left_w, rights, part, lefts, sums):
        plan.run(block[...], left_w[...], rights, lefts, sums)
        part[...] = sums[...].astype(BF16)

    return kernel


def last_kernel(plan, spread, order):
    def kernel(*refs):
        ways, tile = plan.ways, plan.tile
        block, left_w, rights = refs[:3]
        parts, outs = refs[3 : 2 + spread], refs[2 + spread : 2 + spread + spread * ways]
        lefts, sums, held = refs[2 + spread + spread * ways :]
        for step, part in zip(order[:-1], parts):
            held[step] = part[...].astype(F32)
        plan.run(block[...], left_w[...], rights, lefts, held.at[order[-1]])
        row = lax.axis_index("pr")
        place = lax.axis_index("pc")
        line, lane = place // ways, place % ways
        for step in range(spread):
            slot = step_from(line, partner(row, -step, spread), spread)
            for turn in range(ways):
                start = pl.multiple_of(partner(lane, -turn, ways) * tile, 8)
                out = outs[step * ways + turn]
                out[...] = held[slot, pl.ds(start, tile), :].astype(BF16)

    return kernel


def close_kernel(plan, spread, scale):
    def kernel(*refs):
        ways, seconds, firsts, tile = plan.ways, plan.seconds, plan.firsts, plan.tile
        parts, (gate, gain, out_w, out, mixes, ordered) = refs[: spread * ways], refs[spread * ways :]
        lane = lax.axis_index("pc") % ways
        for turn in range(ways):
            total = parts[turn][...].astype(F32)
            for step in range(1, spread):
                total = total + parts[step * ways + turn][...].astype(F32)
            start = pl.multiple_of(partner(lane, turn, ways) * tile, 8)
            mixes[pl.ds(start, tile), :] = total * scale
        for j in range(seconds):
            ordered[j * firsts : (j + 1) * firsts, :] = mixes[pl.ds(j, firsts, stride=seconds), :]
        mixed = ordered[...].astype(BF16).astype(F32)
        centred = mixed - jnp.mean(mixed, axis=-1, keepdims=True)
        power = jnp.mean(centred * centred, axis=-1, keepdims=True)
        scaled = (centred * lax.rsqrt(power + 1e-05) * gain[...]).astype(BF16)
        update = jnp.dot(scaled, out_w[...], preferred_element_type=F32)
        out[...] = (update * gate[...]).astype(out.dtype)

    return kernel


def body(pair_state, left_weight, right_weight, mid_gain, out_weight, out_gate):
    firsts, seconds, width = pair_state.shape
    spread, across = lax.axis_size("pr"), lax.axis_size("pc")
    ways = across // spread
    mixes = left_weight.shape[1]
    rows = seconds * firsts
    plan = Sums(ways, seconds, firsts)
    own = jnp.transpose(pair_state, (1, 0, 2)).reshape(rows, width)

    def send(values, row_step, line_step, lane_step):
        def at(row, line, lane):
            return row * across + line * ways + lane

        pairs = [
            (
                at(
                    partner(row, row_step, spread),
                    partner(line, line_step, spread),
                    partner(lane, lane_step, ways),
                ),
                at(row, line, lane),
            )
            for row in range(spread)
            for line in range(spread)
            for lane in range(ways)
        ]
        return lax.ppermute(values, ("pr", "pc"), pairs)

    def call(kernel, shapes, scratch, name, *operands):
        held = [(x.shape, x.dtype) for x in (*operands, *scratch)] + shapes
        room = sum(math.prod(shape) * jnp.dtype(kind).itemsize for shape, kind in held)
        room = min(2 * room + 4 * 2**20, 60 * 2**20)
        return pl.pallas_call(
            kernel,
            out_shape=[jax.ShapeDtypeStruct(shape, kind) for shape, kind in shapes],
            in_specs=[VMEM] * len(operands),
            out_specs=[VMEM] * len(shapes),
            scratch_shapes=scratch,
            compiler_params=pltpu.CompilerParams(vmem_limit_bytes=room),
            name=name,
        )(*operands)

    moved = {step: send(own, 0, step, 0) for step in range(1, spread)}
    owns = [own] + [send(own, 0, 0, turn) for turn in range(1, ways)]
    order = [0, spread - 1] + [step for step in range(1, spread - 1)]
    part_shape = (ways * plan.tile, mixes)
    rights, part, gate, gain, weight = call(
        open_kernel(plan),
        [
            ((ways * rows, mixes), F32),
            (part_shape, BF16),
            ((rows, width), F32),
            ((1, mixes), F32),
            (out_weight.shape, BF16),
        ],
        plan.scratch,
        "open",
        *owns,
        left_weight,
        right_weight,
        mid_gain.reshape(1, mixes),
        out_weight,
        out_gate,
    )
    parts = [part]
    for step in order[1:-1]:
        parts += call(
            step_kernel(plan),
            [(part_shape, BF16)],
            plan.scratch,
            "step",
            moved[step],
            left_weight,
            rights,
        )
    outs = call(
        last_kernel(plan, spread, order),
        [((plan.tile, mixes), BF16)] * (spread * ways),
        plan.scratch + [pltpu.VMEM((spread,) + part_shape, F32)],
        "last",
        moved[order[-1]],
        left_weight,
        rights,
        *parts,
    )
    met = [
        outs[step * ways + turn] if step == turn == 0 else send(outs[step * ways + turn], step, 0, turn)
        for step in range(spread)
        for turn in range(ways)
    ]
    (update,) = call(
        close_kernel(plan, spread, (spread * firsts) ** -0.5),
        [((rows, width), BF16)],
        [pltpu.VMEM((ways * plan.tile, mixes), F32), pltpu.VMEM((rows, mixes), F32)],
        "close",
        *met,
        gate,
        gain,
        weight,
    )
    return jnp.transpose(update.reshape(seconds, firsts, width), (1, 0, 2))


def solution(mesh):
    placed = (P("pr", "pc", None), P(), P(), P(), P(), P())
    return jax.shard_map(
        body, mesh=mesh, in_specs=placed, out_specs=P("pr", "pc", None), check_vma=False
    )
```

```python
import math

import jax
import jax.numpy as jnp
from jax import lax
from jax.experimental import pallas as pl
from jax.experimental.pallas import tpu as pltpu
from jax.sharding import PartitionSpec as P


VMEM = pl.BlockSpec(memory_space=pltpu.VMEM)
HBM = pl.BlockSpec(memory_space=pltpu.HBM)
F32, BF16 = jnp.float32, jnp.bfloat16


def partner(place, step, count):
    if count & (count - 1) == 0:
        return place ^ abs(step)
    return (place - step) % count


def step_from(place, source, count):
    return place ^ source if count & (count - 1) == 0 else (place - source) % count


def product(block, weight):
    return jnp.dot(block, weight, preferred_element_type=F32).astype(BF16).astype(F32)


class Sums:
    def __init__(self, ways, seconds, firsts):
        self.ways, self.seconds, self.firsts = ways, seconds, firsts
        self.rows = seconds * firsts
        self.tile = seconds * seconds
        self.scratch = [
            pltpu.VMEM((self.rows, 128), F32),
            pltpu.VMEM((ways * self.tile, 128), F32),
        ]

    def run(self, block, weight, rights, lefts, sums):
        seconds, firsts = self.seconds, self.firsts
        lines = self.ways * seconds
        tall, wide, deep = math.gcd(lines, 24), math.gcd(seconds, 12), math.gcd(firsts, 8)
        lefts[...] = product(block, weight)
        for top in range(0, lines, tall):
            for first in range(0, seconds, wide):

                def some(turn, totals):
                    for inner in range(deep):
                        k = turn * deep + inner
                        right = rights[pl.ds(top * firsts + k, tall, stride=firsts), :]
                        totals = tuple(
                            total + right * lefts[pl.ds((first + i) * firsts + k, 1), :]
                            for i, total in enumerate(totals)
                        )
                    return totals

                zero = jnp.zeros((tall, 128), F32)
                totals = lax.fori_loop(0, firsts // deep, some, (zero,) * wide)
                for i, total in enumerate(totals):
                    for lane in range(top // seconds, -(-(top + tall) // seconds)):
                        low = max(top, lane * seconds)
                        high = min(top + tall, (lane + 1) * seconds)
                        at = lane * self.tile + (first + i) * seconds + low - lane * seconds
                        sums[at : at + high - low, :] = total[low - top : high - top]


def open_kernel(plan):
    def kernel(*refs):
        ways, rows = plan.ways, plan.rows
        sources, others = refs[:6], refs[6 : 5 + ways]
        rights, part, gate, left_w, gain, out_w = refs[5 + ways : 11 + ways]
        own, right_w, out_gate, copied, lefts, sums = refs[11 + ways :]
        copies = [
            pltpu.make_async_copy(source, target, copied.at[place])
            for place, (source, target) in enumerate(
                zip(sources, (own, left_w, right_w, out_gate, gain, out_w))
            )
        ]
        for copy in copies:
            copy.start()
        for copy in copies:
            copy.wait()
        lane = lax.axis_index("pc") % ways
        for turn in range(ways):
            block = own if turn == 0 else others[turn - 1]
            start = pl.multiple_of(partner(lane, turn, ways) * rows, 8)
            rights[pl.ds(start, rows), :] = product(block[...], right_w[...])
        plan.run(own[...], left_w[...], rights, lefts, sums)
        part[...] = sums[...].astype(BF16)
        gate[...] = jax.nn.sigmoid(jnp.dot(own[...], out_gate[...], preferred_element_type=F32))

    return kernel


def step_kernel(plan):
    def kernel(block, left_w, rights, part, lefts, sums):
        plan.run(block[...], left_w[...], rights, lefts, sums)
        part[...] = sums[...].astype(BF16)

    return kernel


def last_kernel(plan, spread, order):
    def kernel(*refs):
        ways = plan.ways
        block, left_w, rights = refs[:3]
        parts, outs = refs[3 : 2 + spread], refs[2 + spread : 2 + 2 * spread]
        lefts, held = refs[2 + 2 * spread :]
        for step, part in zip(order[:-1], parts):
            held[step] = part[...].astype(F32)
        plan.run(block[...], left_w[...], rights, lefts, held.at[order[-1]])
        row = lax.axis_index("pr")
        line = lax.axis_index("pc") // ways
        for step in range(spread):
            slot = step_from(line, partner(row, -step, spread), spread)
            outs[step][...] = held[slot].astype(outs[step].dtype)

    return kernel


def meet_kernel(plan, spread, scale):
    def kernel(*refs):
        ways, tile = plan.ways, plan.tile
        parts, outs, total = refs[:spread], refs[spread : spread + ways], refs[spread + ways]
        value = parts[0][...]
        for part in parts[1:]:
            value = value + part[...].astype(F32)
        total[...] = value * scale
        lane = lax.axis_index("pc") % ways
        for turn in range(ways):
            start = pl.multiple_of(partner(lane, -turn, ways) * tile, 8)
            outs[turn][...] = total[pl.ds(start, tile), :].astype(BF16)

    return kernel


def close_kernel(plan):
    def kernel(*refs):
        ways, seconds, firsts, tile = plan.ways, plan.seconds, plan.firsts, plan.tile
        parts, (gate, gain, out_w, out, mixes, ordered) = refs[:ways], refs[ways:]
        lane = lax.axis_index("pc") % ways
        for turn in range(ways):
            start = pl.multiple_of(partner(lane, turn, ways) * tile, 8)
            mixes[pl.ds(start, tile), :] = parts[turn][...].astype(F32)
        for j in range(seconds):
            ordered[j * firsts : (j + 1) * firsts, :] = mixes[pl.ds(j, firsts, stride=seconds), :]
        mixed = ordered[...]
        centred = mixed - jnp.mean(mixed, axis=-1, keepdims=True)
        power = jnp.mean(centred * centred, axis=-1, keepdims=True)
        scaled = (centred * lax.rsqrt(power + 1e-05) * gain[...]).astype(BF16)
        update = jnp.dot(scaled, out_w[...], preferred_element_type=F32)
        out[...] = (update * gate[...]).astype(out.dtype)

    return kernel


def body(pair_state, left_weight, right_weight, mid_gain, out_weight, out_gate):
    firsts, seconds, width = pair_state.shape
    spread, across = lax.axis_size("pr"), lax.axis_size("pc")
    ways = across // spread
    mixes = left_weight.shape[1]
    rows = seconds * firsts
    plan = Sums(ways, seconds, firsts)
    own = jnp.transpose(pair_state, (1, 0, 2)).reshape(rows, width)

    def send(values, row_step, line_step, lane_step):
        def at(row, line, lane):
            return row * across + line * ways + lane

        pairs = [
            (
                at(
                    partner(row, row_step, spread),
                    partner(line, line_step, spread),
                    partner(lane, lane_step, ways),
                ),
                at(row, line, lane),
            )
            for row in range(spread)
            for line in range(spread)
            for lane in range(ways)
        ]
        return lax.ppermute(values, ("pr", "pc"), pairs)

    def call(kernel, shapes, scratch, *operands, far=0):
        sized = [x for x in (*operands, *scratch) if hasattr(x, "dtype") and x.dtype in (F32, BF16)]
        held = [(x.shape, x.dtype) for x in sized] + shapes
        room = sum(math.prod(shape) * jnp.dtype(kind).itemsize for shape, kind in held)
        room = min(2 * room + 4 * 2**20, 60 * 2**20)
        operands = [
            pltpu.with_memory_space_constraint(x, pltpu.HBM) if place < far else x
            for place, x in enumerate(operands)
        ]
        return pl.pallas_call(
            kernel,
            out_shape=[jax.ShapeDtypeStruct(shape, kind) for shape, kind in shapes],
            in_specs=[HBM] * far + [VMEM] * (len(operands) - far),
            out_specs=[VMEM] * len(shapes),
            scratch_shapes=scratch,
            compiler_params=pltpu.CompilerParams(vmem_limit_bytes=room),
        )(*operands)

    moved = {}
    for step in range(spread - 1, 0, -1):
        moved[step] = send(own, 0, step, 0)
    others = []
    for turn in range(1, ways):
        others.append(send(own, 0, 0, turn))
    order = [0, spread - 1] + [step for step in range(1, spread - 1)]
    part_shape = (ways * plan.tile, mixes)
    rights, part, gate, left_w, gain, out_w = call(
        open_kernel(plan),
        [
            ((ways * rows, mixes), F32),
            (part_shape, BF16),
            ((rows, width), F32),
            (left_weight.shape, BF16),
            ((1, mixes), F32),
            (out_weight.shape, BF16),
        ],
        [
            pltpu.VMEM((rows, width), BF16),
            pltpu.VMEM(right_weight.shape, BF16),
            pltpu.VMEM(out_gate.shape, BF16),
            pltpu.SemaphoreType.DMA((6,)),
        ]
        + plan.scratch,
        own,
        left_weight,
        right_weight,
        out_gate,
        mid_gain.reshape(1, mixes),
        out_weight,
        *others,
        far=6,
    )
    parts = [part]
    for step in order[1:-1]:
        parts += call(
            step_kernel(plan), [(part_shape, BF16)], plan.scratch, moved[step], left_w, rights
        )
    outs = call(
        last_kernel(plan, spread, order),
        [(part_shape, F32 if step == 0 else BF16) for step in range(spread)],
        [plan.scratch[0], pltpu.VMEM((spread,) + part_shape, F32)],
        moved[order[-1]],
        left_w,
        rights,
        *parts,
    )
    met = call(
        meet_kernel(plan, spread, (spread * firsts) ** -0.5),
        [((plan.tile, mixes), BF16)] * ways,
        [pltpu.VMEM(part_shape, F32)],
        outs[0],
        *(send(outs[step], step, 0, 0) for step in range(1, spread)),
    )
    (update,) = call(
        close_kernel(plan),
        [((rows, width), BF16)],
        [pltpu.VMEM(part_shape, F32), pltpu.VMEM((rows, mixes), F32)],
        met[0],
        *(send(met[turn], 0, 0, turn) for turn in range(1, ways)),
        gate,
        gain,
        out_w,
    )
    return jnp.transpose(update.reshape(seconds, firsts, width), (1, 0, 2))


def solution(mesh):
    placed = (P("pr", "pc", None), P(), P(), P(), P(), P())

    return jax.shard_map(
        body, mesh=mesh, in_specs=placed, out_specs=P("pr", "pc", None), check_vma=False
    )
```
